32 devices in a mesh: groups: 2 (over y), ctx: 4 (over z), heads: 4 (over x, core).
Axes of the slice: x: 2, y: 2, z: 4, core: 2. Of those that a mesh axis runs over, the one named last changes fastest.
Arguments:
- ssm_input: bfloat16 [2048, 8192], P(('groups', 'ctx'), 'heads'), parts along dimension 0, may hold values from -6 to 6
- decay_log: float32 [2048, 128], P(('groups', 'ctx'), 'heads'), parts along dimension 0
- state_write: bfloat16 [2048, 128], P(('groups', 'ctx')), parts along dimension 0, may hold values from -2 to 2
- state_read: bfloat16 [2048, 128], P(('groups', 'ctx')), parts along dimension 0, may hold values from -2 to 2
- skip_scale: float32 [128], P('heads'), may hold values from 0.5 to 3
- gate_input: bfloat16 [2048, 8192], P(('groups', 'ctx'), 'heads'), parts along dimension 0, may hold values from -6 to 6
- ssm_gain: float32 [8192], P('heads'), may hold values from 0.1 to 1.9
- out_weight: bfloat16 [8192, 4096], P('heads', 'ctx'), may hold values from -0.0625 to 0.0625
- residual_in: bfloat16 [2048, 4096], P(('groups', 'ctx'), 'heads'), parts along dimension 0, may hold values from -24 to 24
- moe_gain: float32 [4096], P('heads'), may hold values from 0.1 to 1.9
- down_latent: bfloat16 [4096, 1024], P('heads'), may hold values from -0.09375 to 0.09375
- expert_up: bfloat16 [8, 1024, 2688], P('ctx', None, 'heads'), may hold values from -0.1875 to 0.1875
- expert_down: bfloat16 [8, 2688, 1024], P('ctx', 'heads'), may hold values from -0.125 to 0.125
- up_latent: bfloat16 [1024, 4096], P(None, 'heads'), may hold values from -0.1875 to 0.1875
- expert_ids: int32 [2048, 22], P(('groups', 'ctx')), parts along dimension 0, may hold values from 0 to 511, as said below
- combine_fixed: int32 [2048, 22], P(('groups', 'ctx')), parts along dimension 0, may hold values from 1 to 65535
Outputs:
- layer_out: bfloat16 [2048, 4096], P(('groups', 'ctx'), 'heads'), parts along dimension 0
The draws below stay inside these ranges and needn't reach their ends.
There are 2 independent parts, one for each index of `groups`. The reference program is written for one: setup_inputs(seed, part) draws one part's arguments, and reference() takes and returns one part's arrays. A program takes and returns all parts, laid end to end along the dimension named above; an argument that names none is the same for every part. Nothing has to cross between parts.
Inputs may be any that keep to these rules, and one draw needn't show every extreme that they name: `expert_ids`: each row names 22 different experts. No expert below 8 is named by more than 16 of the 256 tokens of one block, and in every block some expert below 8 is named by exactly 16 of them.
All inputs are finite; a program needn't handle non-finite values.
Results may differ from the reference program's by a relative error of at most 0.014.
Values may be sent and summed in bfloat16 or wider, within the bound.
A program may use at most 128 MiB of HBM per device.

```python
import jax
import jax.numpy as jnp
from jax import lax

D = 4096
SCAN_HEADS = 128
P_SIZE = 64
N = 128
GRP = 1024
LAT = 1024
FFN = 2688
E = 512
TOPK = 22
TOK_CTX = 256
INNER = 8192
CAP = 16
WAVE = 8
WINDOW_TOKENS = 1024
N_HEADS = 4


def draw_decay_log(key, part):
    key_kind = jax.random.fold_in(key, 21)
    key_fast = jax.random.fold_in(key, 22)
    key_slow = jax.random.fold_in(key, 23)
    key_block = jax.random.fold_in(key, 24)
    key_rough = jax.random.fold_in(key, 25)
    position_key = jax.random.fold_in(key, 26)
    spike_key = jax.random.fold_in(key, 27)
    slow_share = 0.5
    is_slow = jax.random.uniform(key_kind, (SCAN_HEADS,)) < slow_share
    fast_rate = jnp.exp(jax.random.uniform(key_fast, (SCAN_HEADS,), jnp.float32, jnp.log(1.0 / 50.0), jnp.log(1.0 / 30.0)))
    slow_rate = jnp.exp(jax.random.uniform(key_slow, (SCAN_HEADS,), jnp.float32, jnp.log(0.2), jnp.log(0.5))) / WINDOW_TOKENS
    head_rate = jnp.where(is_slow, slow_rate, fast_rate)
    block_factor = jnp.exp(jax.random.uniform(key_block, (WINDOW_TOKENS // TOK_CTX, 1), jnp.float32, jnp.log(0.5), jnp.log(2.0)))
    block_factor = jnp.repeat(block_factor, TOK_CTX, axis=0)
    roughness = jnp.exp(jax.random.uniform(key_rough, (WINDOW_TOKENS, SCAN_HEADS), jnp.float32, jnp.log(0.5), jnp.log(2.0)))
    baseline_rate = head_rate[None, :] * block_factor * roughness
    spike_positions = jax.random.randint(position_key, (2,), 0, WINDOW_TOKENS)
    spike_length = jax.random.uniform(spike_key, (SCAN_HEADS,), jnp.float32, 0.22, 0.69)
    spike_mask = jnp.any(jnp.arange(WINDOW_TOKENS)[:, None] == spike_positions[None, :], axis=1)
    return (baseline_rate + jnp.where(spike_mask[:, None], spike_length[None, :], 0.0)).astype(jnp.float32)


def draw_residual_in(key, part):
    key_row = jax.random.fold_in(key, 31)
    key_col = jax.random.fold_in(key, 32)
    key_base = jax.random.fold_in(key, 33)
    row_scale = jnp.exp(jax.random.uniform(key_row, (WINDOW_TOKENS, 1), jnp.float32, jnp.log(0.3), jnp.log(3.0)))
    position = jnp.arange(D, dtype=jnp.float32)[None, :] / D
    col_scale = 0.5 * 4.0 ** position * jnp.exp(jax.random.uniform(key_col, (1, D), jnp.float32, jnp.log(0.7), jnp.log(1.4)))
    base_value = jax.random.normal(key_base, (WINDOW_TOKENS, D), jnp.float32)
    return jnp.clip(base_value * row_scale * col_scale, -24.0, 24.0).astype(jnp.bfloat16)


def draw_expert_ids(key, part):
    block_count = WINDOW_TOKENS // TOK_CTX
    hot_order = jax.random.permutation(jax.random.fold_in(key, 11), WAVE)
    is_hot = hot_order < max(1, WAVE // 8)
    entries = jnp.arange(WAVE * CAP)
    owner_of = entries // CAP
    copy_index = entries % CAP
    expert_range = jnp.arange(E)

    def one_block(block_key):
        key_load = jax.random.fold_in(block_key, 1)
        key_rows = jax.random.fold_in(block_key, 2)
        key_other = jax.random.fold_in(block_key, 3)
        key_shuffle = jax.random.fold_in(block_key, 4)
        load_count = jax.random.randint(key_load, (WAVE,), CAP // 8, CAP // 2 + 1)
        load_count = jnp.where(is_hot, CAP, load_count)
        is_valid = (copy_index < load_count[owner_of]).astype(jnp.int32)
        ranking = jnp.cumsum(is_valid) - 1
        row_order = jax.random.permutation(key_rows, TOK_CTX)
        target = row_order[jnp.mod(ranking, TOK_CTX)]
        member = jnp.zeros((TOK_CTX, E), jnp.int32).at[target, owner_of].add(is_valid)
        random_part = jax.random.randint(key_other, (TOK_CTX, E), 0, 2 ** 20) * E + expert_range[None, :]
        in_wave = expert_range[None, :] < WAVE
        scores = jnp.where(in_wave, jnp.where(member > 0, 2 ** 30 + expert_range[None, :], -1 - expert_range[None, :]), random_part)
        ignored, chosen = lax.top_k(scores, TOPK)
        shuffle_keys = jax.random.randint(key_shuffle, (TOK_CTX, TOPK), 0, 2 ** 20) * TOPK + jnp.arange(TOPK)[None, :]
        new_order = jnp.argsort(shuffle_keys, axis=1)
        return jnp.take_along_axis(chosen, new_order, axis=1)
    block_keys = jax.random.split(key, block_count)
    return jax.vmap(one_block)(block_keys).reshape(WINDOW_TOKENS, TOPK).astype(jnp.int32)


def place_ends(result, own_key, low, high):
    dims = result.shape
    index_at = [jax.random.randint(jax.random.fold_in(own_key, axis), (), 0, dims[axis]) for axis in range(len(dims))]
    result = result.at[tuple(index_at)].set(low)
    longest = dims.index(max(dims))
    index_at[longest] = (index_at[longest] + 1) % dims[longest]
    return result.at[tuple(index_at)].set(high)


def shard_levels(own_key, dims, cuts, smallest, largest):
    loudness = 1.0
    for dim, blocks in cuts:
        heights = jax.random.uniform(jax.random.fold_in(jax.random.fold_in(own_key, 6), dim), (blocks,), jnp.float32, smallest / len(cuts), largest / len(cuts))
        loudness = loudness * jnp.repeat(jnp.exp(heights), dims[dim] // blocks).reshape((-1,) + (1,) * (len(dims) - 1 - dim))
    return loudness


def gaussian(own_key, dims, scale, limit, cuts=(), kind=jnp.bfloat16):
    factor_of = shard_levels(own_key, dims, cuts, -0.22, 0.18) if cuts else 1.0
    values = jax.random.normal(own_key, dims, jnp.float32) * scale * factor_of
    return jnp.minimum(jnp.maximum(values, -limit), limit).astype(kind)


def setup_inputs(seed: int = 0, part: int = 0) -> dict:
    key_of = jax.random.split(jax.random.key(seed), 17)
    part_splits = jax.random.split(jax.random.fold_in(key_of[16], part), 17)
    return {
        "ssm_input": gaussian(part_splits[0], (WINDOW_TOKENS, INNER), 1.0, 6.0, ((0, 4), (1, 4))),
        "decay_log": draw_decay_log(jax.random.fold_in(jax.random.fold_in(key_of[16], part), 71), part),
        "state_write": gaussian(part_splits[2], (WINDOW_TOKENS, N), 0.3, 2.0, ((0, 4),)),
        "state_read": gaussian(part_splits[3], (WINDOW_TOKENS, N), 0.3, 2.0, ((0, 4),)),
        "skip_scale": jnp.clip(0.5 + 2.5 * jax.random.uniform(key_of[4], (SCAN_HEADS,), jnp.float32) ** shard_levels(key_of[4], (SCAN_HEADS,), ((0, 4),), -0.2, 0.2), 0.5, 3.0),
        "gate_input": gaussian(part_splits[5], (WINDOW_TOKENS, INNER), 1.0, 6.0, ((0, 4), (1, 4))),
        "ssm_gain": jnp.clip(1.0 + 0.18 * jax.random.normal(key_of[6], (INNER,), jnp.float32), 0.1, 1.9),
        "out_weight": gaussian(key_of[7], (INNER, D), INNER ** -0.5, 0.0625, ((0, 4), (1, 4))),
        "residual_in": draw_residual_in(jax.random.fold_in(jax.random.fold_in(key_of[16], part), 71), part),
        "moe_gain": jnp.clip(1.0 + 0.18 * jax.random.normal(key_of[9], (D,), jnp.float32), 0.1, 1.9),
        "down_latent": gaussian(key_of[10], (D, LAT), D ** -0.5, 0.09375, ((0, 4),)),
        "expert_up": gaussian(key_of[11], (WAVE, LAT, FFN), LAT ** -0.5, 0.1875, ((0, 4), (2, 4))),
        "expert_down": gaussian(key_of[12], (WAVE, FFN, LAT), FFN ** -0.5, 0.125, ((0, 4), (1, 4))),
        "up_latent": gaussian(key_of[13], (LAT, D), LAT ** -0.5, 0.1875, ((1, 4),)),
        "expert_ids": draw_expert_ids(jax.random.fold_in(jax.random.fold_in(key_of[16], part), 71), part),
        "combine_fixed": place_ends(jax.random.randint(part_splits[15], (WINDOW_TOKENS, TOPK), 1, 65536), jax.random.fold_in(part_splits[15], 1), 1, 65535).astype(jnp.int32),
    }


epsilon = 1e-05

def ssd_block(carry_state, block_data):
    inputs, decays, writes, reads, writes_low, reads_low = block_data
    cumulative = jnp.cumsum(decays, axis=0)
    length_tok = inputs.shape[0]
    causal = jnp.arange(length_tok)[:, None] >= jnp.arange(length_tok)[None, :]
    spread = jnp.where(causal[:, :, None], cumulative[:, None, :] - cumulative[None, :, :], 0.0)
    intersection = jnp.dot(reads_low, writes_low.T, preferred_element_type=jnp.float32)
    mixing = jnp.where(causal[:, :, None], jnp.exp(-spread), 0.0) * intersection[:, :, None]
    within = jnp.einsum('tsh,shp->thp', mixing, inputs, precision=lax.Precision.HIGHEST)
    carried = jnp.einsum('tn,hnp->thp', reads, carry_state, precision=lax.Precision.HIGHEST) * jnp.exp(-cumulative)[:, :, None]
    tail_decay = jnp.exp(cumulative - cumulative[-1][None, :])
    fresh = jnp.einsum('sn,sh,shp->hnp', writes, tail_decay, inputs, precision=lax.Precision.HIGHEST)
    new_state = carry_state * jnp.exp(-cumulative[-1])[:, None, None] + fresh
    return (new_state, within + carried)

def rms_groups(gated, gain):
    grouped = gated.reshape(gated.shape[0], -1, GRP)
    inv_rms = lax.rsqrt(lax.optimization_barrier(jnp.mean(grouped * grouped, axis=2, keepdims=True)) + epsilon)
    return (grouped * inv_rms).reshape(gated.shape) * gain

def route_tables(ids_block, fixed_block):
    matches = ids_block[:, :, None] == jnp.arange(WAVE)[None, None, :]
    chosen = jnp.any(matches, axis=1).astype(jnp.int32)
    weight_fixed = lax.optimization_barrier(jnp.sum(jnp.where(matches, fixed_block[:, :, None], 0), axis=1))
    slot_index = jnp.cumsum(chosen, axis=0) - 1
    placed = (chosen[:, :, None] == 1) & (slot_index[:, :, None] == jnp.arange(CAP)[None, None, :])
    route_weight = (weight_fixed.astype(jnp.float32) / 65536.0).astype(jnp.bfloat16)
    table = jnp.where(placed, route_weight[:, :, None], jnp.zeros((), jnp.bfloat16)).astype(jnp.bfloat16)
    return (placed.astype(jnp.bfloat16).reshape(TOK_CTX, WAVE * CAP), table.reshape(TOK_CTX, WAVE * CAP))

def expert_apply(operands):
    rows_in, first_mat, second_mat = operands
    hidden = jnp.dot(rows_in, first_mat, preferred_element_type=jnp.float32)
    hidden = (jnp.maximum(hidden, 0.0) ** 2).astype(jnp.bfloat16)
    return jnp.dot(hidden, second_mat, preferred_element_type=jnp.float32).astype(jnp.bfloat16)

def reference(ssm_input, decay_log, state_write, state_read, skip_scale, gate_input, ssm_gain, out_weight, residual_in, moe_gain, down_latent, expert_up, expert_down, up_latent, expert_ids, combine_fixed):
    block_count = WINDOW_TOKENS // TOK_CTX
    inputs = ssm_input.astype(jnp.float32).reshape(block_count, TOK_CTX, SCAN_HEADS, P_SIZE)
    decays = decay_log.astype(jnp.float32).reshape(block_count, TOK_CTX, SCAN_HEADS)
    writes = state_write.astype(jnp.float32).reshape(block_count, TOK_CTX, N)
    reads = state_read.astype(jnp.float32).reshape(block_count, TOK_CTX, N)
    writes_low = state_write.reshape(block_count, TOK_CTX, N)
    reads_low = state_read.reshape(block_count, TOK_CTX, N)
    start_state = jnp.zeros((SCAN_HEADS, N, P_SIZE), jnp.float32)
    ignored, mixed = lax.scan(ssd_block, start_state, (inputs, decays, writes, reads, writes_low, reads_low))
    mixed = mixed.reshape(WINDOW_TOKENS, SCAN_HEADS, P_SIZE) + skip_scale[None, :, None] * inputs.reshape(WINDOW_TOKENS, SCAN_HEADS, P_SIZE)
    gated = mixed.reshape(WINDOW_TOKENS, INNER) * jax.nn.silu(gate_input.astype(jnp.float32))
    normed = rms_groups(gated, ssm_gain).astype(jnp.bfloat16)
    slice_width = INNER // N_HEADS
    mamba_out = jnp.zeros((WINDOW_TOKENS, D), jnp.float32)
    for head_slice in range(N_HEADS):
        lower = head_slice * slice_width
        partial_value = jnp.dot(normed[:, lower:lower + slice_width], out_weight[lower:lower + slice_width], preferred_element_type=jnp.float32)
        partial_value = lax.optimization_barrier(partial_value.astype(jnp.bfloat16))
        mamba_out = mamba_out + partial_value.astype(jnp.float32)
    residual = residual_in.astype(jnp.float32) + mamba_out
    inv_rms = lax.rsqrt(lax.optimization_barrier(jnp.mean(residual * residual, axis=1, keepdims=True)) + epsilon)
    scaled = (residual * moe_gain).astype(jnp.bfloat16)
    latent = (jnp.dot(scaled, down_latent, preferred_element_type=jnp.float32) * inv_rms).astype(jnp.bfloat16)
    placed, tables = jax.vmap(route_tables)(expert_ids.reshape(block_count, TOK_CTX, TOPK), combine_fixed.reshape(block_count, TOK_CTX, TOPK))
    latent_blocks = latent.reshape(block_count, TOK_CTX, LAT)
    dispatched = jax.vmap(lambda place_block, latent_block: jnp.dot(place_block.T, latent_block, preferred_element_type=jnp.float32))(placed, latent_blocks)
    dispatched = dispatched.astype(jnp.bfloat16).reshape(block_count, WAVE, CAP, LAT)
    expert_rows = dispatched.transpose(1, 0, 2, 3).reshape(WAVE, block_count * CAP, LAT)
    expert_out = lax.map(expert_apply, (expert_rows, expert_up, expert_down))
    returned = expert_out.reshape(WAVE, block_count, CAP, LAT).transpose(1, 0, 2, 3).reshape(block_count, WAVE * CAP, LAT)
    combined = jax.vmap(lambda table_block, back_block: jnp.dot(table_block, back_block, preferred_element_type=jnp.float32))(tables, returned)
    combined_low = combined.reshape(WINDOW_TOKENS, LAT).astype(jnp.bfloat16)
    moe_out = jnp.dot(combined_low, up_latent, preferred_element_type=jnp.float32)
    return (residual + moe_out).astype(jnp.bfloat16)
```

```python
import functools

import jax
import jax.numpy as jnp
from jax import lax
from jax.experimental import pallas as pl
from jax.experimental.pallas import tpu as pltpu
from jax.sharding import PartitionSpec as P

D = 4096
GRP = 1024
LAT = 1024
CAP = 16


epsilon = 1e-05


MESH = pl.DeviceIdType.MESH
BF = jnp.bfloat16
F32 = jnp.float32


def vmem(count=1):
    return [pl.BlockSpec(memory_space=pltpu.VMEM)] * count


def greet(device):
    pl.semaphore_signal(
        pltpu.get_barrier_semaphore(), inc=1, device_id=device, device_id_type=MESH
    )


def greeted(count):
    pl.semaphore_wait(pltpu.get_barrier_semaphore(), count)


def one_if(condition):
    return jnp.where(condition, 1, 0)


def remote(src, dst, send, recv, device):
    return pltpu.make_async_remote_copy(
        src_ref=src, dst_ref=dst, send_sem=send, recv_sem=recv, device_id=device, device_id_type=MESH
    )


def pair_wide(first, second, width):
    lane = lax.broadcasted_iota(jnp.int32, (first.shape[0], 2 * width), 1)
    return jnp.where(lane < width, first, second)


def scan_kernel(width, x_ref, col_ref, row_ref, write_ref, read_ref, skip_ref, mixed_ref, state_ref, decay_ref, inter):
    rows = x_ref.shape[0]
    t = lax.broadcasted_iota(jnp.int32, (rows, rows), 0)
    s = lax.broadcasted_iota(jnp.int32, (rows, rows), 1)
    causal = t >= s

    @pl.when(pl.program_id(0) == 0)
    def _():
        product = lax.dot_general(
            read_ref[...], write_ref[...], (((1,), (1,)), ((), ())), preferred_element_type=F32
        )
        inter[...] = jnp.where(causal, product, 0.0)

    x = x_ref[...]
    outs, tails, ends = [], [], []
    for j in range(2):
        col = col_ref[0, :, j : j + 1]
        row = row_ref[0, j : j + 1, :]
        last = row_ref[0, j : j + 1, rows - 1 : rows]
        spread = jnp.where(causal, col - row, 0.0)
        mixing = (jnp.exp(-spread) * inter[...]).astype(BF)
        outs.append(
            jnp.dot(mixing, x[:, j * width : (j + 1) * width], preferred_element_type=F32)
        )
        tails.append(jnp.exp(col - last))
        ends.append(jnp.exp(-last))
    wide = x.astype(F32)
    mixed_ref[...] = jnp.concatenate(outs, axis=1) + skip_ref[...] * wide
    scaled = (wide * pair_wide(tails[0], tails[1], width)).astype(BF)
    state_ref[...] = lax.dot_general(
        write_ref[...], scaled, (((0,), (0,)), ((), ())), preferred_element_type=F32
    )
    decay_ref[...] = pair_wide(ends[0], ends[1], width)


def chain_kernel(n, chunks, state_ref, decay_ref, prior_ref, landed, outgoing, send_sem, recv_sem):
    me = lax.axis_index("ctx")
    size = state_ref.shape[1] // chunks
    has_prev, has_next = me > 0, me < n - 1
    prev, after = jnp.maximum(me - 1, 0), jnp.minimum(me + 1, n - 1)
    pl.when(has_prev)(lambda: greet({"ctx": prev}))
    pl.when(has_next)(lambda: greet({"ctx": after}))
    greeted(one_if(has_prev) + one_if(has_next))

    def copy(k):
        return remote(
            outgoing.at[k], landed.at[k], send_sem.at[k], recv_sem.at[k], {"ctx": after}
        )

    for k in range(chunks):
        part = pl.ds(k * size, size)

        @pl.when(me == 0)
        def _():
            prior_ref[:, part] = jnp.zeros((state_ref.shape[0], size), BF)

            if n > 1:
                outgoing[k] = state_ref[:, part].astype(BF)

        @pl.when(has_prev)
        def _():
            copy(k).wait_recv()
            came = landed[k]
            prior_ref[:, part] = came
            outgoing[k] = (came.astype(F32) * decay_ref[:, part] + state_ref[:, part]).astype(BF)

        pl.when(has_next)(lambda: copy(k).start())
    for k in range(chunks):
        pl.when(has_next)(lambda: copy(k).wait_send())


def gate_kernel(width, mixed_ref, prior_ref, col_ref, read_ref, gate_ref, gain_ref, normed_ref, gated):
    rows = mixed_ref.shape[0]
    pairs = col_ref.shape[0]
    squares = jnp.zeros((rows, 2 * width), F32)
    for p in range(pairs):
        part = slice(p * 2 * width, (p + 1) * 2 * width)
        reach = pair_wide(
            jnp.exp(-col_ref[p, :, 0:1]), jnp.exp(-col_ref[p, :, 1:2]), width
        )
        carried = jnp.dot(read_ref[...], prior_ref[:, part], preferred_element_type=F32) * reach
        gate = gate_ref[:, part].astype(F32)
        value = (mixed_ref[:, part] + carried) * (gate / (1.0 + jnp.exp(-gate)))
        gated[:, part] = value
        squares = squares + value * value
    scale = lax.rsqrt(jnp.sum(squares, axis=1, keepdims=True) / (pairs * 2 * width) + epsilon)
    normed_ref[...] = (gated[...] * scale * gain_ref[...]).astype(BF)


def project_kernel(
    n, heads, normed_ref, weight_ref, out_ref,
    blocks, parts, gathered, summed, final,
    up_send, up_recv, down_send, down_recv, part_send, part_recv, sum_send, sum_recv,
):
    me, head = lax.axis_index("ctx"), lax.axis_index("heads")
    share = n // heads
    column_head = me // share
    rows, width = normed_ref.shape[0], weight_ref.shape[1]
    has_prev, has_next = me > 0, me < n - 1
    prev, after = jnp.maximum(me - 1, 0), jnp.minimum(me + 1, n - 1)

    def holder(j):
        return head * share + j, column_head

    def other(j):
        ctx, side = holder(j)
        return jnp.logical_or(ctx != me, side != head)

    pl.when(has_prev)(lambda: greet({"ctx": prev}))
    pl.when(has_next)(lambda: greet({"ctx": after}))
    for k in range(1, heads):
        greet({"heads": (head + k) % heads})
    count = one_if(has_prev) + one_if(has_next) + heads - 1
    for j in range(share):
        ctx, side = holder(j)
        pl.when(other(j))(lambda: greet({"ctx": ctx, "heads": side}))
        count = count + one_if(other(j))
    greeted(count)

    def upward(s, src):
        return remote(src, blocks.at[me - s], up_send.at[s], up_recv.at[s], {"ctx": after})

    def downward(s, src):
        return remote(src, blocks.at[me + s], down_send.at[s], down_recv.at[s], {"ctx": prev})

    def part_copy(b, target):
        return remote(
            parts.at[b], gathered.at[b % share, head], part_send.at[b],
            part_recv.at[b % share, head], {"heads": target},
        )

    def multiply(b, src):
        step = min(width, 256)
        for lo in range(0, width, step):
            parts[b, :, lo : lo + step] = jnp.dot(
                src[...], weight_ref[:, lo : lo + step], preferred_element_type=F32
            ).astype(BF)
        target = b // share
        pl.when(target != head)(lambda: part_copy(b, target).start())

    pl.when(has_next)(lambda: upward(0, normed_ref).start())
    pl.when(has_prev)(lambda: downward(0, normed_ref).start())
    multiply(me, normed_ref)

    for s in range(1, n):
        low, high = me - s, me + s
        low_ok, high_ok = low >= 0, high < n

        @pl.when(low_ok)
        def _():
            remote(
                normed_ref, blocks.at[low], up_send.at[s - 1], up_recv.at[s - 1], {"ctx": after}
            ).wait_recv()
            pl.when(has_next)(lambda: upward(s, blocks.at[low]).start())
            multiply(low, blocks.at[low])

        @pl.when(high_ok)
        def _():
            remote(
                normed_ref, blocks.at[high], down_send.at[s - 1], down_recv.at[s - 1], {"ctx": prev}
            ).wait_recv()
            pl.when(has_prev)(lambda: downward(s, blocks.at[high]).start())
            multiply(high, blocks.at[high])

    def sum_copy(j):
        ctx, side = holder(j)
        return remote(
            summed.at[j], final.at[me % share], sum_send.at[j], sum_recv.at[me % share],
            {"ctx": ctx, "heads": side},
        )

    for j in range(share):
        mine = head * share + j
        total = parts[mine].astype(F32)
        for k in range(1, heads):
            source = (head + k) % heads
            remote(
                parts.at[mine], gathered.at[j, source], part_send.at[mine],
                part_recv.at[j, source], {"heads": source},
            ).wait_recv()
            total = total + gathered[j, source].astype(F32)
        summed[j] = total.astype(BF)
        pl.when(other(j))(lambda: sum_copy(j).start())

    for i in range(share):
        ctx, side = holder(i)
        here = slice(i * width, (i + 1) * width)

        @pl.when(other(i))
        def _():
            remote(
                summed.at[i], final.at[i], sum_send.at[i], sum_recv.at[i],
                {"ctx": ctx, "heads": side},
            ).wait_recv()
            out_ref[:, here] = final[i].astype(F32)

        @pl.when(jnp.logical_not(other(i)))
        def _():
            out_ref[:, here] = summed[me % share].astype(F32)

    for s in range(n):
        pl.when(jnp.logical_and(has_next, me - s >= 0))(
            lambda: upward(s, normed_ref).wait_send()
        )
        pl.when(jnp.logical_and(has_prev, me + s < n))(
            lambda: downward(s, normed_ref).wait_send()
        )
    for b in range(n):
        pl.when(b // share != head)(lambda: part_copy(b, b // share).wait_send())
    for j in range(share):
        pl.when(other(j))(lambda: sum_copy(j).wait_send())


def slots_kernel(
    n, heads, width, features, src_ref, out_ref,
    first, middle, second, third,
    first_send, first_recv, second_send, second_recv, third_send, third_recv,
):
    me, head = lax.axis_index("ctx"), lax.axis_index("heads")

    for k in range(1, heads):
        greet({"heads": (head + k) % heads})
    for k in range(1, n):
        greet({"ctx": (me + k) % n})
    greeted(heads + n - 2)

    def first_copy(k):
        to = (head + k) % heads
        return remote(
            src_ref.at[to], first.at[k], first_send.at[k], first_recv.at[k], {"heads": to}
        )

    def second_copy(k):
        to = (me + k) % n
        return remote(
            middle.at[to], second.at[me], second_send.at[k], second_recv.at[k], {"ctx": to}
        )

    def third_copy(k):
        to = (head + k) % heads
        return remote(second, third.at[k], third_send.at[k], third_recv.at[k], {"heads": to})

    for k in range(1, heads):
        first_copy(k).start()
    total = src_ref[head].astype(F32)
    for k in range(1, heads):
        first_copy(k).wait_recv()
        total = total + first[k].astype(F32)
    if src_ref.shape[-1] > width:
        power = total[:, :, width : width + 1]
        total = total[:, :, :width] * lax.rsqrt(power / features + epsilon)
    middle[...] = total.astype(BF)
    for k in range(1, n):
        second_copy(k).start()
    second[me] = middle[me]
    for k in range(1, n):
        second_copy(k).wait_recv()
    for k in range(1, heads):
        third_copy(k).start()
    out_ref[head] = second[...]
    for k in range(1, heads):
        third_copy(k).wait_recv()
        out_ref[(head + heads - k) % heads] = third[k]
    for k in range(1, heads):
        first_copy(k).wait_send()
        third_copy(k).wait_send()
    for k in range(1, n):
        second_copy(k).wait_send()


def reaching(collective_id):
    return pltpu.CompilerParams(
        collective_id=collective_id, has_side_effects=True, vmem_limit_bytes=48 * 1024 * 1024
    )


def dma(*shape):
    return pltpu.SemaphoreType.DMA(shape)


def through_slots(pieces, width, features, collective_id):
    heads, n, rows, wide = pieces.shape
    return pl.pallas_call(
        functools.partial(slots_kernel, n, heads, width, features),
        out_shape=jax.ShapeDtypeStruct((heads, n, rows, width), BF),
        in_specs=vmem(),
        out_specs=vmem()[0],
        scratch_shapes=[
            pltpu.VMEM((heads, n, rows, wide), BF),
            pltpu.VMEM((n, rows, width), BF),
            pltpu.VMEM((n, rows, width), BF),
            pltpu.VMEM((heads, n, rows, width), BF),
            dma(heads), dma(heads), dma(n), dma(n), dma(heads), dma(heads),
        ],
        compiler_params=reaching(collective_id),
    )(pieces)


def mixer(ssm_input, decay_log, state_write, state_read, skip_scale, gate_input, ssm_gain):
    n = lax.axis_size("ctx")
    rows, columns = ssm_input.shape
    head_count = decay_log.shape[1]
    width = columns // head_count
    pairs, states = head_count // 2, state_write.shape[1]
    cumulative = jnp.cumsum(decay_log, axis=0)
    by_row = cumulative.T.reshape(pairs, 2, rows)
    by_col = by_row.transpose(0, 2, 1)
    skip = jnp.repeat(skip_scale, width).reshape(1, columns)
    span = 2 * width
    whole = lambda p: (0, 0)
    mixed, state, decay = pl.pallas_call(
        functools.partial(scan_kernel, width),
        grid=(pairs,),
        out_shape=(
            jax.ShapeDtypeStruct((rows, columns), F32),
            jax.ShapeDtypeStruct((states, columns), F32),
            jax.ShapeDtypeStruct((1, columns), F32),
        ),
        in_specs=[
            pl.BlockSpec((rows, span), lambda p: (0, p)),
            pl.BlockSpec((1, rows, 2), lambda p: (p, 0, 0)),
            pl.BlockSpec((1, 2, rows), lambda p: (p, 0, 0)),
            pl.BlockSpec((rows, states), whole),
            pl.BlockSpec((rows, states), whole),
            pl.BlockSpec((1, span), lambda p: (0, p)),
        ],
        out_specs=(
            pl.BlockSpec((rows, span), lambda p: (0, p)),
            pl.BlockSpec((states, span), lambda p: (0, p)),
            pl.BlockSpec((1, span), lambda p: (0, p)),
        ),
        scratch_shapes=[pltpu.VMEM((rows, rows), F32)],
    )(ssm_input, by_col, by_row, state_write, state_read, skip)
    chunks = 4
    prior = pl.pallas_call(
        functools.partial(chain_kernel, n, chunks),
        out_shape=jax.ShapeDtypeStruct((states, columns), BF),
        in_specs=vmem(2),
        out_specs=vmem()[0],
        scratch_shapes=[
            pltpu.VMEM((chunks, states, columns // chunks), BF),
            pltpu.VMEM((chunks, states, columns // chunks), BF),
            dma(chunks),
            dma(chunks),
        ],
        compiler_params=reaching(1),
    )(state, decay)
    group_pairs = GRP // span
    at = lambda g: (0, g)
    return pl.pallas_call(
        functools.partial(gate_kernel, width),
        grid=(columns // GRP,),
        out_shape=jax.ShapeDtypeStruct((rows, columns), BF),
        in_specs=[
            pl.BlockSpec((rows, GRP), at),
            pl.BlockSpec((states, GRP), at),
            pl.BlockSpec((group_pairs, rows, 2), lambda g: (g, 0, 0)),
            pl.BlockSpec((rows, states), whole),
            pl.BlockSpec((rows, GRP), at),
            pl.BlockSpec((1, GRP), at),
        ],
        out_specs=pl.BlockSpec((rows, GRP), at),
        scratch_shapes=[pltpu.VMEM((rows, GRP), F32)],
    )(mixed, prior, by_col, state_read, gate_input, ssm_gain.reshape(1, columns))


def project(normed, weight):
    n, heads = lax.axis_size("ctx"), lax.axis_size("heads")
    rows, width = normed.shape[0], weight.shape[1]
    share = n // heads
    block = (rows, width)
    return pl.pallas_call(
        functools.partial(project_kernel, n, heads),
        out_shape=jax.ShapeDtypeStruct((rows, share * width), F32),
        in_specs=vmem(2),
        out_specs=vmem()[0],
        scratch_shapes=[
            pltpu.VMEM((n,) + normed.shape, BF),
            pltpu.VMEM((n,) + block, BF),
            pltpu.VMEM((share, heads) + block, BF),
            pltpu.VMEM((share,) + block, BF),
            pltpu.VMEM((share,) + block, BF),
            dma(n), dma(n), dma(n), dma(n), dma(n), dma(share, heads), dma(share), dma(share),
        ],
        compiler_params=reaching(2),
    )(normed, weight)


def local(
    ssm_input,
    decay_log,
    state_write,
    state_read,
    skip_scale,
    gate_input,
    ssm_gain,
    out_weight,
    residual_in,
    moe_gain,
    down_latent,
    expert_up,
    expert_down,
    up_latent,
    expert_ids,
    combine_fixed,
):
    row_count = ssm_input.shape[0]
    n, heads = lax.axis_size("ctx"), lax.axis_size("heads")
    features = residual_in.shape[1] * heads
    latent_width = down_latent.shape[1]
    piece = latent_width // heads
    experts_here = expert_up.shape[0]
    wave_size = experts_here * n
    slot_rows = experts_here * CAP

    matches = expert_ids[:, :, None] == jnp.arange(wave_size)[None, None, :]
    chosen = jnp.any(matches, axis=1).astype(jnp.int32)
    weight_fixed = jnp.sum(jnp.where(matches, combine_fixed[:, :, None], 0), axis=1)
    slot_index = jnp.cumsum(chosen, axis=0) - 1
    placed = (chosen[:, :, None] == 1) & (slot_index[:, :, None] == jnp.arange(CAP)[None, None, :])
    route_weight = (weight_fixed.astype(F32) / 65536.0).astype(BF)
    combine_table = jnp.where(placed, route_weight[:, :, None], jnp.zeros((), BF)).reshape(
        row_count, wave_size * CAP
    )
    placed = placed.astype(BF).reshape(row_count, wave_size * CAP)

    normed = mixer(
        ssm_input, decay_log, state_write, state_read, skip_scale, gate_input, ssm_gain
    )
    residual = residual_in.astype(F32) + project(normed, out_weight)
    scaled = (residual * moe_gain).astype(BF)
    latent_part = jnp.dot(scaled, down_latent, preferred_element_type=F32).astype(BF)
    squares = jnp.sum(residual * residual, axis=1).astype(BF)
    side = jnp.concatenate(
        [latent_part, jnp.broadcast_to(squares[:, None], (row_count, 128))], axis=1
    )
    slots = lax.dot_general(
        placed, side, (((0,), (0,)), ((), ())), preferred_element_type=F32
    ).astype(BF)
    slots = slots.reshape(n, slot_rows, latent_width + 128)
    pieces = jnp.stack(
        [
            jnp.concatenate(
                [slots[:, :, h * piece : (h + 1) * piece], slots[:, :, latent_width:]], axis=2
            )
            for h in range(heads)
        ]
    )
    incoming = through_slots(pieces, piece, features, 3)
    incoming = incoming.reshape(heads, n, experts_here, CAP, piece).transpose(2, 1, 3, 0, 4)
    incoming = incoming.reshape(experts_here, n * CAP, latent_width)
    hidden = jnp.einsum("esl,elf->esf", incoming, expert_up, preferred_element_type=F32)
    hidden = (jnp.maximum(hidden, 0.0) ** 2).astype(BF)
    expert_out = jnp.einsum("esf,efl->esl", hidden, expert_down, preferred_element_type=F32)
    expert_out = expert_out.astype(BF).reshape(experts_here, n, CAP, heads, piece)
    expert_out = expert_out.transpose(3, 1, 0, 2, 4).reshape(heads, n, slot_rows, piece)
    returned = through_slots(expert_out, piece, features, 4)
    returned = returned.transpose(1, 2, 0, 3).reshape(wave_size * CAP, latent_width)
    combined = jnp.dot(combine_table, returned, preferred_element_type=F32)
    moe_out = jnp.dot(combined.astype(BF), up_latent, preferred_element_type=F32)
    return (residual + moe_out).astype(BF)


def solution(mesh):
    placed = (
        P(("groups", "ctx"), "heads"),
        P(("groups", "ctx"), "heads"),
        P(("groups", "ctx"), None),
        P(("groups", "ctx"), None),
        P("heads"),
        P(("groups", "ctx"), "heads"),
        P("heads"),
        P("heads", "ctx"),
        P(("groups", "ctx"), "heads"),
        P("heads"),
        P("heads", None),
        P("ctx", None, "heads"),
        P("ctx", "heads", None),
        P(None, "heads"),
        P(("groups", "ctx"), None),
        P(("groups", "ctx"), None),
    )
    return jax.shard_map(
        local, mesh=mesh, in_specs=placed, out_specs=P(("groups", "ctx"), "heads"), check_vma=False
    )
```

```python
import functools

import jax
import jax.numpy as jnp
from jax import lax
from jax.experimental import pallas as pl
from jax.experimental.pallas import tpu as pltpu
from jax.sharding import PartitionSpec as P

D = 4096
GRP = 1024
LAT = 1024
CAP = 16


epsilon = 1e-05


MESH = pl.DeviceIdType.MESH
BF = jnp.bfloat16
F32 = jnp.float32


def vmem(count=1):
    return [pl.BlockSpec(memory_space=pltpu.VMEM)] * count


def greet(device):
    pl.semaphore_signal(
        pltpu.get_barrier_semaphore(), inc=1, device_id=device, device_id_type=MESH
    )


def greeted(count):
    pl.semaphore_wait(pltpu.get_barrier_semaphore(), count)


def one_if(condition):
    return jnp.where(condition, 1, 0)


def remote(src, dst, send, recv, device):
    return pltpu.make_async_remote_copy(
        src_ref=src, dst_ref=dst, send_sem=send, recv_sem=recv, device_id=device, device_id_type=MESH
    )


def pair_wide(first, second, width):
    lane = lax.broadcasted_iota(jnp.int32, (first.shape[0], 2 * width), 1)
    return jnp.where(lane < width, first, second)


def scan_kernel(width, x_ref, col_ref, row_ref, write_ref, read_ref, skip_ref, mixed_ref, state_ref, decay_ref, inter):
    rows = x_ref.shape[0]
    band = rows // 2
    t = lax.broadcasted_iota(jnp.int32, (rows, rows), 0)
    s = lax.broadcasted_iota(jnp.int32, (rows, rows), 1)
    causal = t >= s

    @pl.when(pl.program_id(0) == 0)
    def _():
        product = lax.dot_general(
            read_ref[...], write_ref[...], (((1,), (1,)), ((), ())), preferred_element_type=F32
        )
        inter[...] = jnp.where(causal, product, 0.0)

    x = x_ref[...]
    outs, tails, ends = [], [], []
    for j in range(2):
        col = col_ref[0, :, j : j + 1]
        row = row_ref[0, j : j + 1, :]
        last = row_ref[0, j : j + 1, rows - 1 : rows]
        lane = x[:, j * width : (j + 1) * width]
        bands = []
        for lo in range(0, rows, band):
            hi = lo + band
            spread = jnp.where(causal[lo:hi, lo:hi], col[lo:hi] - row[:, lo:hi], 0.0)
            if lo:
                spread = jnp.concatenate([col[lo:hi] - row[:, :lo], spread], axis=1)
            mixing = (jnp.exp(-spread) * inter[lo:hi, :hi]).astype(BF)
            bands.append(jnp.dot(mixing, lane[:hi], preferred_element_type=F32))
        outs.append(jnp.concatenate(bands, axis=0))
        tails.append(jnp.exp(col - last))
        ends.append(jnp.exp(-last))
    wide = x.astype(F32)
    mixed_ref[...] = jnp.concatenate(outs, axis=1) + skip_ref[...] * wide
    scaled = (wide * pair_wide(tails[0], tails[1], width)).astype(BF)
    state_ref[...] = lax.dot_general(
        write_ref[...], scaled, (((0,), (0,)), ((), ())), preferred_element_type=F32
    )
    decay_ref[...] = pair_wide(ends[0], ends[1], width)


def chain_kernel(n, chunks, state_ref, decay_ref, prior_ref, landed, outgoing, send_sem, recv_sem):
    me = lax.axis_index("ctx")
    size = state_ref.shape[1] // chunks
    has_prev, has_next = me > 0, me < n - 1
    prev, after = jnp.maximum(me - 1, 0), jnp.minimum(me + 1, n - 1)
    pl.when(has_prev)(lambda: greet({"ctx": prev}))
    pl.when(has_next)(lambda: greet({"ctx": after}))
    greeted(one_if(has_prev) + one_if(has_next))

    def copy(k):
        return remote(
            outgoing.at[k], landed.at[k], send_sem.at[k], recv_sem.at[k], {"ctx": after}
        )

    for k in range(chunks):
        part = pl.ds(k * size, size)

        @pl.when(me == 0)
        def _():
            prior_ref[:, part] = jnp.zeros((state_ref.shape[0], size), BF)

            if n > 1:
                outgoing[k] = state_ref[:, part].astype(BF)

        @pl.when(has_prev)
        def _():
            copy(k).wait_recv()
            came = landed[k]
            prior_ref[:, part] = came
            outgoing[k] = (came.astype(F32) * decay_ref[:, part] + state_ref[:, part]).astype(BF)

        pl.when(has_next)(lambda: copy(k).start())
    for k in range(chunks):
        pl.when(has_next)(lambda: copy(k).wait_send())


def gate_kernel(width, mixed_ref, prior_ref, col_ref, read_ref, gate_ref, gain_ref, normed_ref, gated):
    rows = mixed_ref.shape[0]
    pairs = col_ref.shape[0]
    squares = jnp.zeros((rows, 2 * width), F32)
    for p in range(pairs):
        part = slice(p * 2 * width, (p + 1) * 2 * width)
        reach = pair_wide(
            jnp.exp(-col_ref[p, :, 0:1]), jnp.exp(-col_ref[p, :, 1:2]), width
        )
        carried = jnp.dot(read_ref[...], prior_ref[:, part], preferred_element_type=F32) * reach
        gate = gate_ref[:, part].astype(F32)
        value = (mixed_ref[:, part] + carried) * (gate / (1.0 + jnp.exp(-gate)))
        gated[:, part] = value
        squares = squares + value * value
    scale = lax.rsqrt(jnp.sum(squares, axis=1, keepdims=True) / (pairs * 2 * width) + epsilon)
    normed_ref[...] = (gated[...] * scale * gain_ref[...]).astype(BF)


def project_kernel(
    n, heads, normed_ref, weight_ref, out_ref,
    blocks, parts, gathered, summed, final,
    up_send, up_recv, down_send, down_recv, part_send, part_recv, sum_send, sum_recv,
):
    me, head = lax.axis_index("ctx"), lax.axis_index("heads")
    share = n // heads
    column_head = me // share
    rows, width = normed_ref.shape[0], weight_ref.shape[1]
    prev, after = (me + n - 1) % n, (me + 1) % n
    half = rows // 2

    def holder(j):
        return head * share + j, column_head

    def other(j):
        ctx, side = holder(j)
        return jnp.logical_or(ctx != me, side != head)

    greet({"ctx": prev})
    greet({"ctx": after})
    for k in range(1, heads):
        greet({"heads": (head + k) % heads})
    count = heads + 1
    for j in range(share):
        ctx, side = holder(j)
        pl.when(other(j))(lambda: greet({"ctx": ctx, "heads": side}))
        count = count + one_if(other(j))
    greeted(count)

    def up_rows(s):
        return pl.ds(0, half if 2 * s == n else rows)

    def down_rows(s):
        return pl.ds(half, half) if 2 * s == n else pl.ds(0, rows)

    def upward(s, src, block):
        part = up_rows(s)
        return remote(
            src.at[part], blocks.at[block, part], up_send.at[s], up_recv.at[s], {"ctx": after}
        )

    def downward(s, src, block):
        part = down_rows(s)
        return remote(
            src.at[part], blocks.at[block, part], down_send.at[s], down_recv.at[s], {"ctx": prev}
        )

    def part_copy(b, target):
        return remote(
            parts.at[b], gathered.at[b % share, head], part_send.at[b],
            part_recv.at[b % share, head], {"heads": target},
        )

    def multiply(b, src, start, size):
        step = min(width, 256)
        for lo in range(0, width, step):
            parts[b, start : start + size, lo : lo + step] = jnp.dot(
                src[start : start + size, :], weight_ref[:, lo : lo + step],
                preferred_element_type=F32,
            ).astype(BF)

    def deliver(b):
        target = b // share
        pl.when(target != head)(lambda: part_copy(b, target).start())

    reach = n // 2
    upward(1, normed_ref, me).start()
    downward(1, normed_ref, me).start()
    multiply(me, normed_ref, 0, rows)
    deliver(me)
    for s in range(1, reach + 1):
        low, high = (me + n - s) % n, (me + s) % n
        upward(s, normed_ref, low).wait_recv()
        if s < reach:
            upward(s + 1, blocks.at[low], low).start()
        downward(s, normed_ref, high).wait_recv()
        if s < reach:
            downward(s + 1, blocks.at[high], high).start()
            multiply(low, blocks.at[low], 0, rows)
            deliver(low)
            multiply(high, blocks.at[high], 0, rows)
        else:
            multiply(high, blocks.at[high], 0, rows)
        deliver(high)

    def sum_copy(j):
        ctx, side = holder(j)
        return remote(
            summed.at[j], final.at[me % share], sum_send.at[j], sum_recv.at[me % share],
            {"ctx": ctx, "heads": side},
        )

    for j in range(share):
        mine = head * share + j
        total = parts[mine].astype(F32)
        for k in range(1, heads):
            source = (head + k) % heads
            remote(
                parts.at[mine], gathered.at[j, source], part_send.at[mine],
                part_recv.at[j, source], {"heads": source},
            ).wait_recv()
            total = total + gathered[j, source].astype(F32)
        summed[j] = total.astype(BF)
        pl.when(other(j))(lambda: sum_copy(j).start())

    for i in range(share):
        ctx, side = holder(i)
        here = slice(i * width, (i + 1) * width)

        @pl.when(other(i))
        def _():
            remote(
                summed.at[i], final.at[i], sum_send.at[i], sum_recv.at[i],
                {"ctx": ctx, "heads": side},
            ).wait_recv()
            out_ref[:, here] = final[i].astype(F32)

        @pl.when(jnp.logical_not(other(i)))
        def _():
            out_ref[:, here] = summed[me % share].astype(F32)

    for s in range(1, reach + 1):
        upward(s, normed_ref, me).wait_send()
        downward(s, normed_ref, me).wait_send()
    for b in range(n):
        pl.when(b // share != head)(lambda: part_copy(b, b // share).wait_send())
    for j in range(share):
        pl.when(other(j))(lambda: sum_copy(j).wait_send())


def slots_kernel(
    n, heads, width, features, src_ref, out_ref,
    first, middle, second, third,
    first_send, first_recv, second_send, second_recv, third_send, third_recv,
):
    me, head = lax.axis_index("ctx"), lax.axis_index("heads")

    for k in range(1, heads):
        greet({"heads": (head + k) % heads})
    for k in range(1, n):
        greet({"ctx": (me + k) % n})
    greeted(heads + n - 2)

    def first_copy(k):
        to = (head + k) % heads
        return remote(
            src_ref.at[to], first.at[k], first_send.at[k], first_recv.at[k], {"heads": to}
        )

    def second_copy(k):
        to = (me + k) % n
        return remote(
            middle.at[to], second.at[me], second_send.at[k], second_recv.at[k], {"ctx": to}
        )

    def third_copy(k):
        to = (head + k) % heads
        return remote(second, third.at[k], third_send.at[k], third_recv.at[k], {"heads": to})

    for k in range(1, heads):
        first_copy(k).start()
    total = src_ref[head].astype(F32)
    for k in range(1, heads):
        first_copy(k).wait_recv()
        total = total + first[k].astype(F32)
    if src_ref.shape[-1] > width:
        power = total[:, :, width : width + 1]
        total = total[:, :, :width] * lax.rsqrt(power / features + epsilon)
    middle[...] = total.astype(BF)
    for k in range(1, n):
        second_copy(k).start()
    second[me] = middle[me]
    for k in range(1, n):
        second_copy(k).wait_recv()
    for k in range(1, heads):
        third_copy(k).start()
    out_ref[head] = second[...]
    for k in range(1, heads):
        third_copy(k).wait_recv()
        out_ref[(head + heads - k) % heads] = third[k]
    for k in range(1, heads):
        first_copy(k).wait_send()
        third_copy(k).wait_send()
    for k in range(1, n):
        second_copy(k).wait_send()


def reaching(collective_id):
    return pltpu.CompilerParams(
        collective_id=collective_id, has_side_effects=True, vmem_limit_bytes=48 * 1024 * 1024
    )


def dma(*shape):
    return pltpu.SemaphoreType.DMA(shape)


def through_slots(pieces, width, features, collective_id):
    heads, n, rows, wide = pieces.shape
    return pl.pallas_call(
        functools.partial(slots_kernel, n, heads, width, features),
        out_shape=jax.ShapeDtypeStruct((heads, n, rows, width), BF),
        in_specs=vmem(),
        out_specs=vmem()[0],
        scratch_shapes=[
            pltpu.VMEM((heads, n, rows, wide), BF),
            pltpu.VMEM((n, rows, width), BF),
            pltpu.VMEM((n, rows, width), BF),
            pltpu.VMEM((heads, n, rows, width), BF),
            dma(heads), dma(heads), dma(n), dma(n), dma(heads), dma(heads),
        ],
        compiler_params=reaching(collective_id),
    )(pieces)


def mixer(ssm_input, decay_log, state_write, state_read, skip_scale, gate_input, ssm_gain):
    n = lax.axis_size("ctx")
    rows, columns = ssm_input.shape
    head_count = decay_log.shape[1]
    width = columns // head_count
    pairs, states = head_count // 2, state_write.shape[1]
    cumulative = jnp.cumsum(decay_log, axis=0)
    by_row = cumulative.T.reshape(pairs, 2, rows)
    by_col = by_row.transpose(0, 2, 1)
    skip = jnp.repeat(skip_scale, width).reshape(1, columns)
    span = 2 * width
    whole = lambda p: (0, 0)
    mixed, state, decay = pl.pallas_call(
        functools.partial(scan_kernel, width),
        grid=(pairs,),
        out_shape=(
            jax.ShapeDtypeStruct((rows, columns), F32),
            jax.ShapeDtypeStruct((states, columns), F32),
            jax.ShapeDtypeStruct((1, columns), F32),
        ),
        in_specs=[
            pl.BlockSpec((rows, span), lambda p: (0, p)),
            pl.BlockSpec((1, rows, 2), lambda p: (p, 0, 0)),
            pl.BlockSpec((1, 2, rows), lambda p: (p, 0, 0)),
            pl.BlockSpec((rows, states), whole),
            pl.BlockSpec((rows, states), whole),
            pl.BlockSpec((1, span), lambda p: (0, p)),
        ],
        out_specs=(
            pl.BlockSpec((rows, span), lambda p: (0, p)),
            pl.BlockSpec((states, span), lambda p: (0, p)),
            pl.BlockSpec((1, span), lambda p: (0, p)),
        ),
        scratch_shapes=[pltpu.VMEM((rows, rows), F32)],
    )(ssm_input, by_col, by_row, state_write, state_read, skip)
    chunks = 8
    prior = pl.pallas_call(
        functools.partial(chain_kernel, n, chunks),
        out_shape=jax.ShapeDtypeStruct((states, columns), BF),
        in_specs=vmem(2),
        out_specs=vmem()[0],
        scratch_shapes=[
            pltpu.VMEM((chunks, states, columns // chunks), BF),
            pltpu.VMEM((chunks, states, columns // chunks), BF),
            dma(chunks),
            dma(chunks),
        ],
        compiler_params=reaching(1),
    )(state, decay)
    group_pairs = GRP // span
    at = lambda g: (0, g)
    return pl.pallas_call(
        functools.partial(gate_kernel, width),
        grid=(columns // GRP,),
        out_shape=jax.ShapeDtypeStruct((rows, columns), BF),
        in_specs=[
            pl.BlockSpec((rows, GRP), at),
            pl.BlockSpec((states, GRP), at),
            pl.BlockSpec((group_pairs, rows, 2), lambda g: (g, 0, 0)),
            pl.BlockSpec((rows, states), whole),
            pl.BlockSpec((rows, GRP), at),
            pl.BlockSpec((1, GRP), at),
        ],
        out_specs=pl.BlockSpec((rows, GRP), at),
        scratch_shapes=[pltpu.VMEM((rows, GRP), F32)],
    )(mixed, prior, by_col, state_read, gate_input, ssm_gain.reshape(1, columns))


def project(normed, weight):
    n, heads = lax.axis_size("ctx"), lax.axis_size("heads")
    rows, width = normed.shape[0], weight.shape[1]
    share = n // heads
    block = (rows, width)
    return pl.pallas_call(
        functools.partial(project_kernel, n, heads),
        out_shape=jax.ShapeDtypeStruct((rows, share * width), F32),
        in_specs=vmem(2),
        out_specs=vmem()[0],
        scratch_shapes=[
            pltpu.VMEM((n,) + normed.shape, BF),
            pltpu.VMEM((n,) + block, BF),
            pltpu.VMEM((share, heads) + block, BF),
            pltpu.VMEM((share,) + block, BF),
            pltpu.VMEM((share,) + block, BF),
            dma(n), dma(n), dma(n), dma(n), dma(n), dma(share, heads), dma(share), dma(share),
        ],
        compiler_params=reaching(2),
    )(normed, weight)


def local(
    ssm_input,
    decay_log,
    state_write,
    state_read,
    skip_scale,
    gate_input,
    ssm_gain,
    out_weight,
    residual_in,
    moe_gain,
    down_latent,
    expert_up,
    expert_down,
    up_latent,
    expert_ids,
    combine_fixed,
):
    row_count = ssm_input.shape[0]
    n, heads = lax.axis_size("ctx"), lax.axis_size("heads")
    features = residual_in.shape[1] * heads
    latent_width = down_latent.shape[1]
    piece = latent_width // heads
    experts_here = expert_up.shape[0]
    wave_size = experts_here * n
    slot_rows = experts_here * CAP

    matches = expert_ids[:, :, None] == jnp.arange(wave_size)[None, None, :]
    chosen = jnp.any(matches, axis=1).astype(jnp.int32)
    weight_fixed = jnp.sum(jnp.where(matches, combine_fixed[:, :, None], 0), axis=1)
    slot_index = jnp.cumsum(chosen, axis=0) - 1
    placed = (chosen[:, :, None] == 1) & (slot_index[:, :, None] == jnp.arange(CAP)[None, None, :])
    route_weight = (weight_fixed.astype(F32) / 65536.0).astype(BF)
    combine_table = jnp.where(placed, route_weight[:, :, None], jnp.zeros((), BF)).reshape(
        row_count, wave_size * CAP
    )
    placed = placed.astype(BF).reshape(row_count, wave_size * CAP)

    normed = mixer(
        ssm_input, decay_log, state_write, state_read, skip_scale, gate_input, ssm_gain
    )
    residual = residual_in.astype(F32) + project(normed, out_weight)
    scaled = (residual * moe_gain).astype(BF)
    latent_part = jnp.dot(scaled, down_latent, preferred_element_type=F32).astype(BF)
    squares = jnp.sum(residual * residual, axis=1).astype(BF)
    side = jnp.concatenate(
        [latent_part, jnp.broadcast_to(squares[:, None], (row_count, 128))], axis=1
    )
    slots = lax.dot_general(
        placed, side, (((0,), (0,)), ((), ())), preferred_element_type=F32
    ).astype(BF)
    slots = slots.reshape(n, slot_rows, latent_width + 128)
    pieces = jnp.stack(
        [
            jnp.concatenate(
                [slots[:, :, h * piece : (h + 1) * piece], slots[:, :, latent_width:]], axis=2
            )
            for h in range(heads)
        ]
    )
    incoming = through_slots(pieces, piece, features, 3)
    incoming = incoming.reshape(heads, n, experts_here, CAP, piece).transpose(2, 1, 3, 0, 4)
    incoming = incoming.reshape(experts_here, n * CAP, latent_width)
    hidden = jnp.einsum("esl,elf->esf", incoming, expert_up, preferred_element_type=F32)
    hidden = (jnp.maximum(hidden, 0.0) ** 2).astype(BF)
    expert_out = jnp.einsum("esf,efl->esl", hidden, expert_down, preferred_element_type=F32)
    expert_out = expert_out.astype(BF).reshape(experts_here, n, CAP, heads, piece)
    expert_out = expert_out.transpose(3, 1, 0, 2, 4).reshape(heads, n, slot_rows, piece)
    returned = through_slots(expert_out, piece, features, 4)
    returned = returned.transpose(1, 2, 0, 3).reshape(wave_size * CAP, latent_width)
    combined = jnp.dot(combine_table, returned, preferred_element_type=F32)
    moe_out = jnp.dot(combined.astype(BF), up_latent, preferred_element_type=F32)
    return (residual + moe_out).astype(BF)


def solution(mesh):
    placed = (
        P(("groups", "ctx"), "heads"),
        P(("groups", "ctx"), "heads"),
        P(("groups", "ctx"), None),
        P(("groups", "ctx"), None),
        P("heads"),
        P(("groups", "ctx"), "heads"),
        P("heads"),
        P("heads", "ctx"),
        P(("groups", "ctx"), "heads"),
        P("heads"),
        P("heads", None),
        P("ctx", None, "heads"),
        P("ctx", "heads", None),
        P(None, "heads"),
        P(("groups", "ctx"), None),
        P(("groups", "ctx"), None),
    )
    return jax.shard_map(
        local, mesh=mesh, in_specs=placed, out_specs=P(("groups", "ctx"), "heads"), check_vma=False
    )
```
